32 devices in a mesh: groups: 2 (over x), facet: 16 (over z, y, core).
Axes of the slice: x: 2, y: 2, z: 4, core: 2. Of those that a mesh axis runs over, the one named last changes fastest.
Arguments:
- sky_strips: bfloat16 [2, 16, 16384], P(None, 'groups', 'facet'), parts along dimension 1, may hold values from -6 to 6
- prolate: float32 [1024], replicated, may hold values from 0.25 to 1
- subgrid_offset: int32 [16], replicated, may hold values from 0 to 16383
- owner: int32 [16], replicated, may hold values from 0 to 15, as said below
- observed: float32 [64, 2, 8, 8192], P(('groups', 'facet')), parts along dimension 0, may hold values from -6 to 6
- vis_uv: float32 [64, 8192], P(('groups', 'facet')), parts along dimension 0, may hold values from 0 to 512
- vis_count: int32 [64], P(('groups', 'facet')), parts along dimension 0, may hold values from 1 to 8192
Outputs:
- residual_vis: bfloat16 [64, 2, 8, 8192], P(('groups', 'facet')), parts along dimension 0
- image_update: float32 [2, 16, 16384], P(None, 'groups', 'facet'), parts along dimension 1
The draws below stay inside these ranges and needn't reach their ends.
There are 2 independent parts, one for each index of `groups`. The reference program is written for one: setup_inputs(seed, part) draws one part's arguments, and reference() takes and returns one part's arrays. A program takes and returns all parts, laid end to end along the dimension named above; an argument that names none is the same for every part. Nothing has to cross between parts.
Inputs may be any that keep to these rules, and one draw needn't show every extreme that they name: `owner`: each index of facet owns at most 2 subgrids, and some index owns exactly 2.
All inputs are finite; a program needn't handle non-finite values.
Results may differ from the reference program's by a relative error of at most 0.01.
Values may be sent and summed in bfloat16 or wider, within the bound.
No kernel may reach another device: no remote copies, remote signals or barrier semaphores. Data moves between devices by JAX's collectives and lax.ppermute only.
A program may use at most 64 MiB of HBM per device.

```python
import math
import jax
import jax.numpy as jnp
from jax import lax

FACET_WIDTH = 1024
POINTS = 512
ROWS = 8
VIS = 8192
SLOTS = 2
SUBGRIDS = 16
SLOT_TOTAL = 32
GRID = 16384
N_FACET = 16


def draw_owner(key, part):
    stream = jax.random.fold_in(key, 11)
    first_key, second_key, third_key = jax.random.split(stream, 3)
    others = jax.random.permutation(first_key, SLOT_TOTAL - 2)[:SUBGRIDS - 2] + 2
    chosen = jnp.concatenate([jnp.array([0, 1], dtype=jnp.int32), others.astype(jnp.int32)])
    chosen = chosen[jax.random.permutation(second_key, SUBGRIDS)]
    relabel = jax.random.permutation(third_key, N_FACET).astype(jnp.int32)
    return relabel[chosen // SLOTS]


def with_ends(result, stream_key, smallest, largest):
    place = [jax.random.randint(jax.random.fold_in(stream_key, axis), (), 0, length) for axis, length in enumerate(result.shape)]
    widest = result.shape.index(max(result.shape))
    next_to = place[:widest] + [(place[widest] + 1) % result.shape[widest]] + place[widest + 1:]
    return result.at[tuple(place)].set(smallest).at[tuple(next_to)].set(largest)


def block_levels(own_key, extent, cuts, low, largest):
    factor_of, own = 1.0, jax.random.fold_in(own_key, 6)
    for dim, parts in cuts:
        heights = jnp.exp(jax.random.uniform(jax.random.fold_in(own, dim), (parts,), jnp.float32, low / len(cuts), largest / len(cuts)))
        factor_of = factor_of * jnp.repeat(heights, extent[dim] // parts).reshape([-1 if axis == dim else 1 for axis in range(len(extent))])
    return factor_of


def gaussian(rng, extent, scale, limit, shards=(), kind=jnp.bfloat16):
    values = scale * jax.random.normal(rng, extent, jnp.float32)
    if shards:
        values = values * block_levels(rng, extent, shards, -0.22, 0.18)
    return jnp.clip(values, -limit, limit).astype(kind)


def setup_inputs(seed: int = 0, part: int = 0) -> dict:
    streams_of = jax.random.split(jax.random.key(seed), 8)
    part_splits = jax.random.split(jax.random.fold_in(streams_of[7], part), 8)
    return {
        "sky_strips": gaussian(part_splits[0], (2, ROWS, GRID), 1.0, 6.0, ((2, 16),)),
        "prolate": jnp.clip(jnp.exp(jax.random.uniform(streams_of[1], (FACET_WIDTH,), jnp.float32, math.log(0.25), math.log(1.0))), 0.25, 1.0),
        "subgrid_offset": with_ends(jax.random.randint(streams_of[2], (SUBGRIDS,), 0, GRID), jax.random.fold_in(streams_of[2], 1), 0, GRID - 1).astype(jnp.int32),
        "owner": draw_owner(jax.random.fold_in(streams_of[7], 71), part),
        "observed": gaussian(part_splits[4], (SLOT_TOTAL, 2, ROWS, VIS), 1.0, 6.0, ((0, 16),), jnp.float32),
        "vis_uv": jnp.clip(512.0 * jax.random.uniform(part_splits[5], (SLOT_TOTAL, VIS), jnp.float32) ** block_levels(part_splits[5], (SLOT_TOTAL, VIS), ((0, 16),), -0.2, 0.2), 0.0, 512.0),
        "vis_count": with_ends(jax.random.randint(part_splits[6], (SLOT_TOTAL,), 1, VIS + 1), jax.random.fold_in(part_splits[6], 1), 1, VIS).astype(jnp.int32),
    }


TWO_PI = 6.283185307179586

def matmul(first, second):
    return jnp.dot(first.astype(jnp.float32), second.astype(jnp.float32), precision=lax.Precision.HIGHEST)

def modular_product(factor, second, modulus):
    upper = second // 256
    lower = second % 256
    return (factor * lower % modulus + factor * upper % modulus * 256 % modulus) % modulus

def phasor(index, modulus):
    angle = index.astype(jnp.float32) * (TWO_PI / modulus)
    return (jnp.cos(angle), jnp.sin(angle))

def forward_table(columns, points, modulus):
    across = jnp.arange(columns, dtype=jnp.int32)[:, None]
    along = jnp.arange(points, dtype=jnp.int32)[None, :]
    cosine, sine = phasor(modular_product(across, along, modulus), modulus)
    upper_half = jnp.concatenate([cosine, -sine], 1)
    lower_half = jnp.concatenate([sine, cosine], 1)
    return jnp.concatenate([upper_half, lower_half], 0).astype(jnp.bfloat16)

def facet_terms(strip_re, strip_im, weight, columns, anchor, offsets, phase_table, modulus, points, product):
    scaled_re = strip_re * weight
    scaled_im = strip_im * weight
    cosine, sine = phasor(modular_product(columns[None, :], offsets[:, None], modulus), modulus)
    mod_re = scaled_re[None] * cosine[:, None] + scaled_im[None] * sine[:, None]
    mod_im = scaled_im[None] * cosine[:, None] - scaled_re[None] * sine[:, None]
    subgrid_count = offsets.shape[0]
    strip_rows = strip_re.shape[0]
    modulated = jnp.concatenate([mod_re, mod_im], -1).astype(jnp.bfloat16).reshape(subgrid_count * strip_rows, -1)
    raw = product(modulated, phase_table).reshape(subgrid_count, strip_rows, 2 * points)
    along = jnp.arange(points, dtype=jnp.int32)
    shifted = (along[None, :] + offsets[:, None]) % modulus
    out_cos, out_sin = phasor(modular_product(anchor, shifted, modulus), modulus)
    raw_re = raw[..., :points]
    raw_im = raw[..., points:]
    factor_scale = 1.0 / math.sqrt(modulus)
    term_re = (raw_re * out_cos[:, None] + raw_im * out_sin[:, None]) * factor_scale
    term_im = (raw_im * out_cos[:, None] - raw_re * out_sin[:, None]) * factor_scale
    return jnp.concatenate([term_re, term_im], -1)

def slot_layout(owner, slots, total):
    subgrid_count = owner.shape[0]
    index = jnp.arange(subgrid_count, dtype=jnp.int32)
    same = owner[:, None] == owner[None, :]
    before = index[None, :] < index[:, None]
    ranked = lax.optimization_barrier(jnp.sum(same & before, axis=1)).astype(jnp.int32)
    slot_of = owner.astype(jnp.int32) * slots + ranked
    wanted = jnp.arange(total, dtype=jnp.int32)
    matches = slot_of[None, :] == wanted[:, None]
    is_held = jnp.any(matches, axis=1)
    slot_ids = lax.optimization_barrier(jnp.sum(jnp.where(matches, index[None, :], 0), axis=1)).astype(jnp.int32)
    return (slot_ids, is_held)

def degrid_slot(grid, observed_slot, coords, live_count, is_held, block, points, product):
    strip_rows = grid.shape[0]
    total = coords.shape[0]
    blocks = total // block
    obs_blocks = observed_slot.reshape(2, strip_rows, blocks, block).transpose(2, 0, 1, 3)
    coord_blocks = coords.reshape(blocks, block)
    along = jnp.arange(points, dtype=jnp.int32).astype(jnp.float32)
    within = jnp.arange(block, dtype=jnp.int32)

    def visit(carry, inputs):
        position, coord_block, obs_block = inputs
        turns = along[:, None] * coord_block[None, :] / points
        fraction = turns - jnp.floor(turns)
        cosine = jnp.cos(TWO_PI * fraction)
        sine = jnp.sin(TWO_PI * fraction)
        degrid_table = jnp.concatenate([jnp.concatenate([cosine, sine], 1), jnp.concatenate([-sine, cosine], 1)], 0).astype(jnp.bfloat16)
        model = product(grid, degrid_table) / math.sqrt(points)
        live = (position * block + within < live_count) & is_held
        resid_re = jnp.where(live[None, :], obs_block[0] - model[:, :block], jnp.float32(0.0))
        resid_im = jnp.where(live[None, :], obs_block[1] - model[:, block:], jnp.float32(0.0))
        residual = jnp.concatenate([resid_re, resid_im], -1).astype(jnp.bfloat16)
        carry = carry + product(residual, degrid_table.T)
        return (carry, residual)
    initial = jnp.zeros((strip_rows, 2 * points), jnp.float32)
    total_sum, residuals = lax.scan(visit, initial, (jnp.arange(blocks, dtype=jnp.int32), coord_blocks, obs_blocks))
    update = (total_sum / math.sqrt(total)).astype(jnp.bfloat16)
    resid_re = residuals[..., :block].transpose(1, 0, 2).reshape(strip_rows, total)
    resid_im = residuals[..., block:].transpose(1, 0, 2).reshape(strip_rows, total)
    return (update, jnp.stack([resid_re, resid_im], 0))

def lift_back(updates, slot_ids, offsets, anchor, phase_table, modulus, points, product):
    number = updates.shape[0]
    strip_rows = updates.shape[1]
    subgrid_count = offsets.shape[0]
    chosen = lax.optimization_barrier(jnp.sum(jnp.where(slot_ids[:, None] == jnp.arange(subgrid_count, dtype=jnp.int32)[None, :], offsets[None, :], 0), axis=1)).astype(jnp.int32)
    along = jnp.arange(points, dtype=jnp.int32)
    cosine, sine = phasor(modular_product(anchor, (along[None, :] + chosen[:, None]) % modulus, modulus), modulus)
    upd_re = updates[..., :points].astype(jnp.float32)
    upd_im = updates[..., points:].astype(jnp.float32)
    lift_re = upd_re * cosine[:, None] - upd_im * sine[:, None]
    lift_im = upd_re * sine[:, None] + upd_im * cosine[:, None]
    lifted = jnp.concatenate([lift_re, lift_im], -1).astype(jnp.bfloat16).reshape(number * strip_rows, 2 * points)
    width = phase_table.shape[0] // 2
    back = product(lifted, phase_table.T).reshape(number, strip_rows, 2 * width)
    across = jnp.arange(width, dtype=jnp.int32)
    col_cos, col_sin = phasor(modular_product(across[None, :], chosen[:, None], modulus), modulus)
    back_re = back[..., :width]
    back_im = back[..., width:]
    out_re = lax.optimization_barrier(jnp.sum(back_re * col_cos[:, None] - back_im * col_sin[:, None], axis=0))
    out_im = lax.optimization_barrier(jnp.sum(back_re * col_sin[:, None] + back_im * col_cos[:, None], axis=0))
    return jnp.concatenate([out_re, out_im], -1)

def reference(sky_strips, prolate, subgrid_offset, owner, observed, vis_uv, vis_count):
    modulus = FACET_WIDTH * N_FACET
    phase_table = forward_table(FACET_WIDTH, POINTS, modulus)
    columns = jnp.arange(FACET_WIDTH, dtype=jnp.int32)
    offsets = subgrid_offset.astype(jnp.int32)

    def accumulate(total, facet):
        anchor = facet * FACET_WIDTH
        strip = lax.dynamic_slice_in_dim(sky_strips, anchor, FACET_WIDTH, 2).astype(jnp.float32)
        terms = facet_terms(strip[0], strip[1], prolate, columns, anchor, offsets, phase_table, modulus, POINTS, matmul)
        return (total + terms, None)
    initial = jnp.zeros((SUBGRIDS, ROWS, 2 * POINTS), jnp.float32)
    summed, _ = lax.scan(accumulate, initial, jnp.arange(N_FACET, dtype=jnp.int32))
    subgrids = summed.astype(jnp.bfloat16)
    slot_ids, is_held = slot_layout(offsets * 0 + owner.astype(jnp.int32), SLOTS, SLOT_TOTAL)
    grids = jnp.take(subgrids, slot_ids, axis=0)
    block = min(1024, VIS)

    def degrid_one(inputs):
        grid, obs_slot, coords, live_count, held_flag = inputs
        return degrid_slot(grid, obs_slot, coords, live_count, held_flag, block, POINTS, matmul)
    updates, residual_vis = lax.map(degrid_one, (grids, observed, vis_uv, vis_count.astype(jnp.int32), is_held))

    def facet_image(facet):
        return lift_back(updates, slot_ids, offsets, facet * FACET_WIDTH, phase_table, modulus, POINTS, matmul)
    images = lax.map(facet_image, jnp.arange(N_FACET, dtype=jnp.int32))
    weight = jnp.concatenate([prolate, prolate]) / math.sqrt(SUBGRIDS * POINTS)
    images = images * weight
    image_update = images.reshape(N_FACET, ROWS, 2, FACET_WIDTH).transpose(2, 1, 0, 3).reshape(2, ROWS, modulus)
    return (residual_vis, image_update)
```

```python
import functools
import math

import jax
import jax.numpy as jnp
from jax import lax
from jax.experimental import pallas as pl
from jax.experimental.pallas import tpu as pltpu
from jax.sharding import PartitionSpec as P

POINTS = 512
FINE = 8
COARSE = POINTS // FINE
BLOCK = 2 * COARSE
ROOT = 8
STEP = 64
CHUNK = 1024

COS = (
    0.9999999890590217, -4.934801124863452, 4.058694841243232, -1.3351584301691248,
    0.23502980840046309, -0.025358983639642813, 0.001593910683444594,
)
SIN = (
    3.14159265125575, -5.167712550664621, 2.550160355805489, -0.5992423074495862,
    0.08208188864038139, -0.00727531575291481, 0.00039528045693413335,
)


def horner(coefficients, z):
    total = coefficients[-1] * z + coefficients[-2]
    for value in coefficients[-3::-1]:
        total = total * z + value
    return total


def turn(t):
    y = 2.0 * (t - jnp.floor(t + 0.5))
    z = y * y
    return horner(COS, z), horner(SIN, z) * y


def modular(first, second, modulus):
    if modulus & (modulus - 1) == 0:
        return (first * second) & (modulus - 1)
    upper = second // 256
    lower = second % 256
    return (first * lower % modulus + first * upper % modulus * 256 % modulus) % modulus


def iota(shape, axis):
    return lax.broadcasted_iota(jnp.int32, shape, axis)


def column_points(shape):
    column = iota(shape, 1)
    return (column % COARSE) * FINE + column // BLOCK, (column // COARSE) % 2


def facet_at(position, me, facets):
    bits = facets.bit_length() - 1
    flipped = position * 0
    for bit in range(bits):
        flipped = flipped | (((position >> bit) & 1) << (bits - 1 - bit))
    return flipped ^ me


def swap(block):
    return pltpu.roll(block, COARSE, 1)


def blocks_of(value):
    return [value[:, b * BLOCK : (b + 1) * BLOCK] for b in range(FINE)]


def prepare_kernel(modulus, slots, uv_ref, table_ref, coarse_ref, fine_ref, v_re, v_im, u_re, u_im):
    width = table_ref.shape[0] // 2
    points, part = column_points(v_re.shape)
    fraction = modular(iota(v_re.shape, 0), points, modulus).astype(jnp.float32) * (1.0 / modulus)
    v_re[...], v_im[...] = turn(fraction + 0.25 * part.astype(jnp.float32))
    points, _ = column_points(u_re.shape)
    fraction = modular(iota(u_re.shape, 0) * STEP, points, modulus).astype(jnp.float32) * (1.0 / modulus)
    u_re[...], u_im[...] = turn(fraction)

    def table_step(step, _):
        c = u_re[pl.ds(step, 1), :]
        s = u_im[pl.ds(step, 1), :]
        row = pl.multiple_of(step * STEP, STEP)
        table_ref[pl.ds(row, STEP), :] = (v_re[...] * c - v_im[...] * s).astype(jnp.bfloat16)
        table_ref[pl.ds(width + row, STEP), :] = (v_re[...] * s + v_im[...] * c).astype(jnp.bfloat16)
        return 0

    lax.fori_loop(0, width // STEP, table_step, 0)

    total = uv_ref.shape[1]
    chunk = min(512, total)

    for slot in range(slots):

        def coarse_step(step, _):
            at = pl.ds(pl.multiple_of(step * chunk, chunk), chunk)
            u = jnp.broadcast_to(uv_ref[slot : slot + 1, at], (ROOT, chunk))
            fine = u * (1.0 / POINTS)
            fine_ref[slot, 0, :, at], fine_ref[slot, 1, :, at] = turn(fine)
            low = u * (FINE / POINTS)
            low = low - jnp.floor(low)
            re, im = turn(low * iota(u.shape, 0).astype(jnp.float32))
            c, s = turn(u * (FINE * ROOT / POINTS))
            for pair in range(ROOT // 2):
                next_re = re * c - im * s
                next_im = re * s + im * c
                rows = pair * 2 * ROOT
                coarse_ref[slot, rows : rows + 2 * ROOT, at] = jnp.concatenate(
                    [re, next_re], 0
                ).astype(jnp.bfloat16)
                coarse_ref[slot, COARSE + rows : COARSE + rows + 2 * ROOT, at] = jnp.concatenate(
                    [im, next_im], 0
                ).astype(jnp.bfloat16)
                re = next_re * c - next_im * s
                im = next_re * s + next_im * c
            return 0

        lax.fori_loop(0, total // chunk, coarse_step, 0)


def visibility_kernel(
    modulus,
    facets,
    me_ref,
    owner_ref,
    offset_ref,
    count_ref,
    sky_ref,
    prolate_ref,
    table_ref,
    coarse_ref,
    fine_ref,
    observed_ref,
    residual_ref,
    update_ref,
    lhs,
    raw,
    mod_c,
    mod_s,
    turn_c,
    turn_s,
):
    me = me_ref[0]
    slots = count_ref.shape[0]
    rows = sky_ref.shape[2]
    width = sky_ref.shape[3]
    subgrids = owner_ref.shape[0]

    def find(index, carry):
        held, offsets = carry
        mine = owner_ref[index] == me
        offsets = tuple(
            jnp.where(mine & (held == slot), offset_ref[index], offsets[slot]) for slot in range(slots)
        )
        return held + mine.astype(jnp.int32), offsets

    zero = jnp.int32(0)
    held, offsets = lax.fori_loop(0, subgrids, find, (zero, (zero,) * slots))

    facet = facet_at(iota((facets, width), 0), me, facets)
    across = facet * width + iota((facets, width), 1)
    for slot in range(slots):
        fraction = modular(across, offsets[slot], modulus).astype(jnp.float32) * (1.0 / modulus)
        c, s = turn(fraction)
        mod_c[slot] = c * prolate_ref[...]
        mod_s[slot] = s * prolate_ref[...]

    points, part = column_points((facets, FINE * BLOCK))
    facet = facet_at(iota(points.shape, 0), me, facets)
    c, s = turn(modular(facet, points, facets).astype(jnp.float32) * (1.0 / facets))
    scale = 1.0 / math.sqrt(modulus)
    turn_c[...] = c * scale
    turn_s[...] = jnp.where(part == 0, -s, s) * scale

    for slot in range(slots):

        def modulate(pair, _):
            parts = []
            for which in range(2):
                position = pair * 2 + which
                c = mod_c[slot, pl.ds(position, 1), :]
                s = mod_s[slot, pl.ds(position, 1), :]
                re = sky_ref[position, 0].astype(jnp.float32)
                im = sky_ref[position, 1].astype(jnp.float32)
                parts.append((re * c + im * s, im * c - re * s))
            row = pl.multiple_of((slot * facets + pair * 2) * rows, 2 * rows)
            at = pl.ds(row, 2 * rows)
            lhs[at, :width] = jnp.concatenate([parts[0][0], parts[1][0]], 0).astype(jnp.bfloat16)
            lhs[at, width:] = jnp.concatenate([parts[0][1], parts[1][1]], 0).astype(jnp.bfloat16)
            return 0

        lax.fori_loop(0, facets // 2, modulate, 0)

    raw[...] = jnp.dot(lhs[...], table_ref[...], preferred_element_type=jnp.float32)

    total = observed_ref.shape[3]
    chunk = min(CHUNK, total)
    first_half = jnp.where(iota((rows, BLOCK), 1) < COARSE, jnp.float32(1.0), jnp.float32(-1.0))

    for slot in range(slots):

        def add_facet(position, carry):
            straight, crossed = carry
            row = pl.multiple_of((slot * facets + position) * rows, rows)
            value = raw[pl.ds(row, rows), :]
            return (
                straight + value * turn_c[pl.ds(position, 1), :],
                crossed + value * turn_s[pl.ds(position, 1), :],
            )

        empty = jnp.zeros((rows, FINE * BLOCK), jnp.float32)
        straight, crossed = lax.fori_loop(0, facets, add_facet, (empty, empty))
        grid = [
            (first + swap(second)).astype(jnp.bfloat16).astype(jnp.float32)
            for first, second in zip(blocks_of(straight), blocks_of(crossed))
        ]
        points_lhs = jnp.concatenate(
            [block * first_half for block in grid] + [swap(block) for block in grid], 0
        ).astype(jnp.bfloat16)
        live = jnp.where(slot < held, count_ref[slot], 0)

        def visit(step, carry):
            at = pl.ds(pl.multiple_of(step * chunk, chunk), chunk)
            coarse = coarse_ref[slot, :, at]
            c = fine_ref[slot, 0, :, at]
            s = fine_ref[slot, 1, :, at]
            terms = jnp.dot(points_lhs, coarse, preferred_element_type=jnp.float32)
            half = FINE * rows
            re = terms[half - rows : half]
            im = terms[2 * half - rows :]
            for b in range(FINE - 2, -1, -1):
                re, im = (
                    terms[b * rows : (b + 1) * rows] + (re * c - im * s),
                    terms[half + b * rows : half + (b + 1) * rows] + (re * s + im * c),
                )
            scale = 1.0 / math.sqrt(POINTS)
            alive = step * chunk + iota((rows, chunk), 1) < live
            re = jnp.where(alive, observed_ref[slot, 0, :, at] - re * scale, 0.0).astype(jnp.bfloat16)
            im = jnp.where(alive, observed_ref[slot, 1, :, at] - im * scale, 0.0).astype(jnp.bfloat16)
            residual_ref[slot, 0, :, at] = re
            residual_ref[slot, 1, :, at] = im
            re = re.astype(jnp.float32)
            im = im.astype(jnp.float32)
            all_re, all_im = [re], [im]
            for b in range(1, FINE):
                re, im = re * c + im * s, im * c - re * s
                all_re.append(re)
                all_im.append(im)
            spread = jnp.concatenate(all_re + all_im, 0).astype(jnp.bfloat16)
            return carry + lax.dot_general(
                spread, coarse, (((1,), (1,)), ((), ())), preferred_element_type=jnp.float32
            )

        gathered = lax.fori_loop(
            0, total // chunk, visit, jnp.zeros((2 * FINE * rows, BLOCK), jnp.float32)
        )
        scale = 1.0 / math.sqrt(total)
        for b in range(FINE):
            re = gathered[b * rows : (b + 1) * rows]
            im = gathered[(FINE + b) * rows : (FINE + b + 1) * rows]
            update_ref[slot, :, b * BLOCK : (b + 1) * BLOCK] = (
                (swap(im) + re * first_half) * scale
            ).astype(jnp.bfloat16)


def image_kernel(
    modulus,
    facets,
    slots,
    me_ref,
    owner_ref,
    offset_ref,
    update_ref,
    prolate_ref,
    table_ref,
    image_ref,
    lhs,
    mod_c,
    mod_s,
    taken,
    place,
):
    me = me_ref[0]
    subgrids = owner_ref.shape[0]
    rows = update_ref.shape[1]
    width = image_ref.shape[2]

    def clear(index, _):
        taken[index] = 0
        return 0

    lax.fori_loop(0, facets, clear, 0)

    def assign(index, _):
        holder = owner_ref[index]
        rank = taken[holder]
        taken[holder] = rank + 1
        place[index] = facet_at(holder ^ me, 0, facets) * slots + rank
        return 0

    lax.fori_loop(0, subgrids, assign, 0)

    across = me * width + iota((subgrids, width), 1)
    fraction = modular(across, jnp.broadcast_to(offset_ref[...], across.shape), modulus)
    mod_c[...], mod_s[...] = turn(fraction.astype(jnp.float32) * (1.0 / modulus))

    points, part = column_points((rows, FINE * BLOCK))
    straight, crossed = turn(modular(me, points, facets).astype(jnp.float32) * (1.0 / facets))
    crossed = jnp.where(part == 0, -crossed, crossed)

    def lift(pair, _):
        parts = []
        for which in range(2):
            value = update_ref[place[pair * 2 + which]].astype(jnp.float32)
            turned = jnp.concatenate([swap(block) for block in blocks_of(value)], 1)
            parts.append(value * straight + turned * crossed)
        at = pl.ds(pl.multiple_of(pair * 2 * rows, 2 * rows), 2 * rows)
        lhs[at, :] = jnp.concatenate(parts, 0).astype(jnp.bfloat16)
        return 0

    lax.fori_loop(0, subgrids // 2, lift, 0)
    back = lax.dot_general(
        lhs[...], table_ref[...], (((1,), (1,)), ((), ())), preferred_element_type=jnp.float32
    )
    out_re = jnp.zeros((rows, width), jnp.float32)
    out_im = jnp.zeros((rows, width), jnp.float32)
    for index in range(subgrids):
        re = back[index * rows : (index + 1) * rows, :width]
        im = back[index * rows : (index + 1) * rows, width:]
        c = mod_c[index : index + 1, :]
        s = mod_s[index : index + 1, :]
        out_re = out_re + (re * c - im * s)
        out_im = out_im + (re * s + im * c)
    weight = prolate_ref[...] * (1.0 / math.sqrt(subgrids * POINTS))
    image_ref[0] = out_re * weight
    image_ref[1] = out_im * weight


def gather(value, facets):
    together = value[None]
    distance = facets // 2
    while distance:
        pairs = [(index, index ^ distance) for index in range(facets)]
        together = jnp.concatenate([together, lax.ppermute(together, "facet", pairs)], 0)
        distance //= 2
    return together


VMEM = pl.BlockSpec(memory_space=pltpu.VMEM)
SMEM = pl.BlockSpec(memory_space=pltpu.SMEM)


def call(kernel, inputs, outputs, scratch, name):
    return pl.pallas_call(
        kernel,
        in_specs=inputs,
        out_specs=jax.tree.map(lambda _: VMEM, outputs),
        out_shape=outputs,
        scratch_shapes=scratch,
        name=name,
        compiler_params=pltpu.CompilerParams(vmem_limit_bytes=40 << 20),
    )


def local(facets, sky_strips, prolate, subgrid_offset, owner, observed, vis_uv, vis_count):
    parts, rows, width = sky_strips.shape
    slots, _, _, total = observed.shape
    subgrids = owner.shape[0]
    modulus = width * facets
    shape = jax.ShapeDtypeStruct
    me = lax.axis_index("facet").astype(jnp.int32).reshape(1)
    weight = prolate.reshape(1, width)

    table, coarse, fine = call(
        functools.partial(prepare_kernel, modulus, slots),
        [VMEM],
        (
            shape((2 * width, 2 * POINTS), jnp.bfloat16),
            shape((slots, BLOCK, total), jnp.bfloat16),
            shape((slots, 2, rows, total), jnp.float32),
        ),
        [pltpu.VMEM((STEP, 2 * POINTS), jnp.float32)] * 2
        + [pltpu.VMEM((width // STEP, 2 * POINTS), jnp.float32)] * 2,
        "prepare",
    )(vis_uv)

    sky = gather(sky_strips, facets)
    residual, update = call(
        functools.partial(visibility_kernel, modulus, facets),
        [SMEM] * 4 + [VMEM] * 6,
        (
            shape((slots, 2, rows, total), jnp.bfloat16),
            shape((slots, rows, 2 * POINTS), jnp.bfloat16),
        ),
        [
            pltpu.VMEM((slots * facets * rows, 2 * width), jnp.bfloat16),
            pltpu.VMEM((slots * facets * rows, 2 * POINTS), jnp.float32),
        ]
        + [pltpu.VMEM((slots, facets, width), jnp.float32)] * 2
        + [pltpu.VMEM((facets, 2 * POINTS), jnp.float32)] * 2,
        "visibility",
    )(me, owner, subgrid_offset, vis_count, sky, weight, table, coarse, fine, observed)

    updates = gather(update, facets).reshape(facets * slots, rows, 2 * POINTS)
    image = call(
        functools.partial(image_kernel, modulus, facets, slots),
        [SMEM, SMEM] + [VMEM] * 4,
        shape((2, rows, width), jnp.float32),
        [pltpu.VMEM((subgrids * rows, 2 * POINTS), jnp.bfloat16)]
        + [pltpu.VMEM((subgrids, width), jnp.float32)] * 2
        + [pltpu.SMEM((facets,), jnp.int32), pltpu.SMEM((subgrids,), jnp.int32)],
        "image",
    )(me, owner, subgrid_offset.reshape(subgrids, 1), updates, weight, table)
    return residual, image


def solution(mesh):
    in_specs = (
        P(None, "groups", "facet"),
        P(),
        P(),
        P(),
        P(("groups", "facet"), None, None, None),
        P(("groups", "facet"), None),
        P(("groups", "facet")),
    )
    out_specs = (P(("groups", "facet"), None, None, None), P(None, "groups", "facet"))
    return jax.shard_map(
        functools.partial(local, mesh.shape["facet"]),
        mesh=mesh,
        in_specs=in_specs,
        out_specs=out_specs,
        check_vma=False,
    )
```

```python
import functools
import math

import jax
import jax.numpy as jnp
from jax import lax
from jax.experimental import pallas as pl
from jax.experimental.pallas import tpu as pltpu
from jax.sharding import PartitionSpec as P


POINTS = 512
FINE = 8
COARSE = POINTS // FINE
BLOCK = 2 * COARSE
ROOT = 8
STEP = 64
FAR = 4
CHUNK = 512

COS = (
    0.9999999890590217, -4.934801124863452, 4.058694841243232, -1.3351584301691248,
    0.23502980840046309, -0.025358983639642813, 0.001593910683444594,
)
SIN = (
    3.14159265125575, -5.167712550664621, 2.550160355805489, -0.5992423074495862,
    0.08208188864038139, -0.00727531575291481, 0.00039528045693413335,
)


def horner(coefficients, z):
    total = coefficients[-1] * z + coefficients[-2]
    for value in coefficients[-3::-1]:
        total = total * z + value
    return total


def turn(t):
    y = 2.0 * (t - jnp.floor(t + 0.5))
    z = y * y
    return horner(COS, z), horner(SIN, z) * y


def modular(first, second, modulus):
    if modulus & (modulus - 1) == 0:
        return (first * second) & (modulus - 1)
    upper = second // 256
    lower = second % 256
    return (first * lower % modulus + first * upper % modulus * 256 % modulus) % modulus


def iota(shape, axis):
    return lax.broadcasted_iota(jnp.int32, shape, axis)


def column_points(shape):
    column = iota(shape, 1)
    return (column % COARSE) * FINE + column // BLOCK, (column // COARSE) % 2


def facet_at(position, me, facets):
    far = min(FAR, facets)
    near = facets // far
    bits = near.bit_length() - 1
    flipped = me & (near - 1)
    for bit in range(bits):
        flipped = flipped ^ (((position // far >> bit) & 1) << (bits - 1 - bit))
    return (me // near - position % far + far) % far * near + flipped


def position_of(facet, me, facets):
    far = min(FAR, facets)
    near = facets // far
    bits = near.bit_length() - 1
    flipped = 0
    for bit in range(bits):
        flipped = flipped | ((((facet ^ me) >> bit) & 1) << (bits - 1 - bit))
    return (me // near - facet // near + far) % far + far * flipped


def swap(block):
    return pltpu.roll(block, COARSE, 1)


def blocks_of(value):
    return [value[:, b * BLOCK : (b + 1) * BLOCK] for b in range(FINE)]


def find_offsets(me, owner_ref, offset_ref, slots):
    def find(index, carry):
        held, offsets = carry
        mine = owner_ref[index] == me
        offsets = tuple(
            jnp.where(mine & (held == slot), offset_ref[index], offsets[slot]) for slot in range(slots)
        )
        return held + mine.astype(jnp.int32), offsets

    zero = jnp.int32(0)
    return lax.fori_loop(0, owner_ref.shape[0], find, (zero, (zero,) * slots))


def fraction_of(first, second, modulus):
    return modular(first, second, modulus).astype(jnp.float32) * (1.0 / modulus)


def fetch(copies, semaphores):
    started = [
        pltpu.make_async_copy(source, target, semaphores.at[index])
        for index, (source, target) in enumerate(copies)
    ]
    for copy in started:
        copy.start()
    for copy in started:
        copy.wait()


def setup_kernel(
    modulus,
    slots,
    sky_hbm,
    owner_hbm,
    offset_hbm,
    count_hbm,
    prolate_hbm,
    sky_ref,
    mod_ref,
    turn_ref,
    live_ref,
    owner_ref,
    offset_ref,
    count_ref,
    prolate_ref,
    semaphores,
):
    fetch(
        (
            (sky_hbm, sky_ref),
            (owner_hbm, owner_ref),
            (offset_hbm, offset_ref),
            (count_hbm, count_ref),
            (prolate_hbm, prolate_ref),
        ),
        semaphores,
    )
    me = lax.axis_index("facet")
    facets, width = mod_ref.shape[2:]
    held, offsets = find_offsets(me, owner_ref, offset_ref, slots)
    weight = prolate_ref[...]

    facet = facet_at(iota((facets, width), 0), me, facets)
    across = facet * width + iota((facets, width), 1)
    for slot in range(slots):
        c, s = turn(fraction_of(across, offsets[slot], modulus))
        mod_ref[0, slot] = c * weight
        mod_ref[1, slot] = s * weight
        live_ref[slot] = jnp.full(live_ref.shape[1:], jnp.where(slot < held, count_ref[slot], 0))

    points, part = column_points((facets, 2 * POINTS))
    facet = facet_at(iota(points.shape, 0), me, facets)
    c, s = turn(fraction_of(facet, points, facets))
    scale = 1.0 / math.sqrt(modulus)
    turn_ref[0] = c * scale
    turn_ref[1] = jnp.where(part == 0, -s, s) * scale


def plan_kernel(
    modulus,
    owner_hbm,
    offset_hbm,
    prolate_hbm,
    residual_ref,
    back_ref,
    lift_ref,
    residual_hbm,
    owner_ref,
    offset_ref,
    prolate_ref,
    semaphores,
):
    leaving = pltpu.make_async_copy(residual_ref, residual_hbm, semaphores.at[3])
    leaving.start()
    fetch(
        ((owner_hbm, owner_ref), (offset_hbm, offset_ref), (prolate_hbm, prolate_ref)), semaphores
    )
    me = lax.axis_index("facet")
    facets = lax.axis_size("facet")
    subgrids, width = back_ref.shape[1:]
    row = iota((subgrids, 128), 0)

    def place_offset(index, placed):
        return jnp.where(row == index, offset_ref[index], placed)

    column = lax.fori_loop(0, subgrids, place_offset, jnp.zeros(row.shape, jnp.int32), unroll=True)
    across = me * width + iota((subgrids, width), 1)
    c, s = turn(fraction_of(across, jnp.concatenate([column] * (width // 128), 1), modulus))
    weight = prolate_ref[...] * (1.0 / math.sqrt(subgrids * POINTS))
    back_ref[0] = c * weight
    back_ref[1] = s * weight

    points, part = column_points(lift_ref.shape[1:])
    c, s = turn(fraction_of(me, points, facets))
    lift_ref[0] = c
    lift_ref[1] = jnp.where(part == 0, -s, s)
    leaving.wait()


def table_kernel(modulus, table_ref, v_re, v_im, u_re, u_im):
    width = table_ref.shape[0] // 2
    points, part = column_points(v_re.shape)
    fraction = fraction_of(iota(v_re.shape, 0), points, modulus)
    v_re[...], v_im[...] = turn(fraction + 0.25 * part.astype(jnp.float32))
    points, _ = column_points(u_re.shape)
    u_re[...], u_im[...] = turn(fraction_of(iota(u_re.shape, 0) * STEP, points, modulus))

    def table_step(step, _):
        c = u_re[pl.ds(step, 1), :]
        s = u_im[pl.ds(step, 1), :]
        row = pl.multiple_of(step * STEP, STEP)
        table_ref[pl.ds(row, STEP), :] = (v_re[...] * c - v_im[...] * s).astype(jnp.bfloat16)
        table_ref[pl.ds(width + row, STEP), :] = (v_re[...] * s + v_im[...] * c).astype(jnp.bfloat16)
        return 0

    lax.fori_loop(0, width // STEP, table_step, 0)


def back_table_kernel(modulus, table_ref, v_re, v_im, u_re, u_im):
    width = table_ref.shape[1] // 2
    row = iota(v_re.shape, 0)
    fraction = fraction_of(iota(v_re.shape, 1), row % COARSE * FINE, modulus)
    v_re[...], v_im[...] = turn(fraction + 0.25 * (row // COARSE).astype(jnp.float32))
    u_re[...], u_im[...] = turn(fraction_of(iota(u_re.shape, 1), iota(u_re.shape, 0), modulus))

    def table_step(b, _):
        c = u_re[pl.ds(b, 1), :]
        s = u_im[pl.ds(b, 1), :]
        at = pl.ds(pl.multiple_of(b * BLOCK, BLOCK), BLOCK)
        table_ref[at, :width] = (v_re[...] * c - v_im[...] * s).astype(jnp.bfloat16)
        table_ref[at, width:] = (v_re[...] * s + v_im[...] * c).astype(jnp.bfloat16)
        return 0

    lax.fori_loop(0, FINE, table_step, 0)


def coarse_kernel(slot, uv_ref, coarse_ref, fine_ref):
    total = uv_ref.shape[1]
    chunk = min(512, total)

    def coarse_step(step, _):
        at = pl.ds(pl.multiple_of(step * chunk, chunk), chunk)
        u = jnp.broadcast_to(uv_ref[slot : slot + 1, at], (ROOT, chunk))
        fine = u * (1.0 / POINTS)
        fine_ref[0, :, at], fine_ref[1, :, at] = turn(fine)
        low = u * (FINE / POINTS)
        low = low - jnp.floor(low)
        re, im = turn(low * iota(u.shape, 0).astype(jnp.float32))
        c, s = turn(u * (FINE * ROOT / POINTS))
        for pair in range(ROOT // 2):
            next_re = re * c - im * s
            next_im = re * s + im * c
            rows = pair * 2 * ROOT
            coarse_ref[rows : rows + 2 * ROOT, at] = jnp.concatenate(
                [re, next_re], 0
            ).astype(jnp.bfloat16)
            coarse_ref[COARSE + rows : COARSE + rows + 2 * ROOT, at] = jnp.concatenate(
                [im, next_im], 0
            ).astype(jnp.bfloat16)
            re = next_re * c - next_im * s
            im = next_re * s + next_im * c
        return 0

    lax.fori_loop(0, total // chunk, coarse_step, 0)


def grid_kernel(facets, sky_ref, mod_ref, turn_ref, table_ref, points_ref, lhs, raw):
    slots = mod_ref.shape[1]
    rows = sky_ref.shape[2]
    width = sky_ref.shape[3]

    for slot in range(slots):

        def modulate(pair, _):
            parts = []
            for which in range(2):
                position = pair * 2 + which
                c = mod_ref[0, slot, pl.ds(position, 1), :]
                s = mod_ref[1, slot, pl.ds(position, 1), :]
                re = sky_ref[position, 0].astype(jnp.float32)
                im = sky_ref[position, 1].astype(jnp.float32)
                parts.append((re * c + im * s, im * c - re * s))
            row = pl.multiple_of((slot * facets + pair * 2) * rows, 2 * rows)
            at = pl.ds(row, 2 * rows)
            lhs[at, :width] = jnp.concatenate([parts[0][0], parts[1][0]], 0).astype(jnp.bfloat16)
            lhs[at, width:] = jnp.concatenate([parts[0][1], parts[1][1]], 0).astype(jnp.bfloat16)
            return 0

        lax.fori_loop(0, facets // 2, modulate, 0, unroll=True)

    raw[...] = jnp.dot(lhs[...], table_ref[...], preferred_element_type=jnp.float32)
    first_half = jnp.where(iota((rows, BLOCK), 1) < COARSE, jnp.float32(1.0), jnp.float32(-1.0))

    for slot in range(slots):

        def add_facet(position, carry):
            straight, crossed = carry
            row = pl.multiple_of((slot * facets + position) * rows, rows)
            value = raw[pl.ds(row, rows), :]
            return (
                straight + value * turn_ref[0, pl.ds(position, 1), :],
                crossed + value * turn_ref[1, pl.ds(position, 1), :],
            )

        empty = jnp.zeros((rows, FINE * BLOCK), jnp.float32)
        straight, crossed = lax.fori_loop(0, facets, add_facet, (empty, empty), unroll=True)
        grid = [
            (first + swap(second)).astype(jnp.bfloat16).astype(jnp.float32)
            for first, second in zip(blocks_of(straight), blocks_of(crossed))
        ]
        points_ref[slot] = jnp.concatenate(
            [block * first_half for block in grid] + [swap(block) for block in grid], 0
        ).astype(jnp.bfloat16)


def visibility_kernel(slots, points_ref, live_ref, observed_ref, *refs):
    coarse_refs, fine_refs = refs[:slots], refs[slots : 2 * slots]
    residual_ref, update_ref = refs[2 * slots :]
    _, _, rows, total = observed_ref.shape
    chunk = min(CHUNK, total)
    first_half = jnp.where(iota((rows, BLOCK), 1) < COARSE, jnp.float32(1.0), jnp.float32(-1.0))

    for slot in range(slots):
        points_lhs = points_ref[slot]
        live = jnp.concatenate([live_ref[slot]] * (chunk // live_ref.shape[2]), 1)

        def visit(step, carry):
            at = pl.ds(pl.multiple_of(step * chunk, chunk), chunk)
            coarse = coarse_refs[slot][:, at]
            c = fine_refs[slot][0, :, at]
            s = fine_refs[slot][1, :, at]
            terms = jnp.dot(points_lhs, coarse, preferred_element_type=jnp.float32)
            half = FINE * rows
            re = terms[half - rows : half]
            im = terms[2 * half - rows :]
            for b in range(FINE - 2, -1, -1):
                re, im = (
                    terms[b * rows : (b + 1) * rows] + (re * c - im * s),
                    terms[half + b * rows : half + (b + 1) * rows] + (re * s + im * c),
                )
            scale = 1.0 / math.sqrt(POINTS)
            alive = step * chunk + iota((rows, chunk), 1) < live
            re = jnp.where(alive, observed_ref[slot, 0, :, at] - re * scale, 0.0).astype(jnp.bfloat16)
            im = jnp.where(alive, observed_ref[slot, 1, :, at] - im * scale, 0.0).astype(jnp.bfloat16)
            residual_ref[slot, 0, :, at] = re
            residual_ref[slot, 1, :, at] = im
            re = re.astype(jnp.float32)
            im = im.astype(jnp.float32)
            all_re, all_im = [re], [im]
            for _ in range(1, FINE):
                re, im = re * c + im * s, im * c - re * s
                all_re.append(re)
                all_im.append(im)
            spread = jnp.concatenate(all_re + all_im, 0).astype(jnp.bfloat16)
            return carry + lax.dot_general(
                spread, coarse, (((1,), (1,)), ((), ())), preferred_element_type=jnp.float32
            )

        gathered = lax.fori_loop(
            0, total // chunk, visit, jnp.zeros((2 * FINE * rows, BLOCK), jnp.float32), unroll=True
        )
        scale = 1.0 / math.sqrt(total)
        for b in range(FINE):
            re = gathered[b * rows : (b + 1) * rows]
            im = gathered[(FINE + b) * rows : (FINE + b + 1) * rows]
            update_ref[slot, :, b * BLOCK : (b + 1) * BLOCK] = (
                (swap(im) + re * first_half) * scale
            ).astype(jnp.bfloat16)


def image_kernel(
    facets,
    slots,
    owner_ref,
    update_ref,
    back_ref,
    lift_ref,
    table_ref,
    image_ref,
    lhs,
    taken,
    place,
):
    me = lax.axis_index("facet")
    subgrids = owner_ref.shape[0]
    rows = update_ref.shape[1]
    width = image_ref.shape[2]

    def clear(index, _):
        taken[index] = 0
        return 0

    lax.fori_loop(0, facets, clear, 0, unroll=True)

    def assign(index, _):
        holder = owner_ref[index]
        rank = taken[holder]
        taken[holder] = rank + 1
        place[index] = position_of(holder, me, facets) * slots + rank
        return 0

    lax.fori_loop(0, subgrids, assign, 0, unroll=True)

    straight = lift_ref[0]
    crossed = lift_ref[1]

    def lift(pair, _):
        parts = []
        for which in range(2):
            value = update_ref[place[pair * 2 + which]].astype(jnp.float32)
            turned = jnp.concatenate([swap(block) for block in blocks_of(value)], 1)
            parts.append(value * straight + turned * crossed)
        at = pl.ds(pl.multiple_of(pair * 2 * rows, 2 * rows), 2 * rows)
        lhs[at, :] = jnp.concatenate(parts, 0).astype(jnp.bfloat16)
        return 0

    lax.fori_loop(0, subgrids // 2, lift, 0, unroll=True)
    back = jnp.dot(lhs[...], table_ref[...], preferred_element_type=jnp.float32)
    out_re = jnp.zeros((rows, width), jnp.float32)
    out_im = jnp.zeros((rows, width), jnp.float32)
    for index in range(subgrids):
        re = back[index * rows : (index + 1) * rows, :width]
        im = back[index * rows : (index + 1) * rows, width:]
        c = back_ref[0, index : index + 1, :]
        s = back_ref[1, index : index + 1, :]
        out_re = out_re + (re * c - im * s)
        out_im = out_im + (re * s + im * c)
    image_ref[0] = out_re
    image_ref[1] = out_im


def gather(value, staged, facets):
    far = min(FAR, facets)
    near = facets // far
    pieces = [staged[None]]
    for step in range(1, far):
        pairs = [(index, (index + step * near) % facets) for index in range(facets)]
        pieces.append(lax.ppermute(value, "facet", pairs)[None])
    together = jnp.concatenate(pieces, 0)
    distance = near // 2
    while distance:
        pairs = [(index, index ^ distance) for index in range(facets)]
        received = lax.ppermute(together, "facet", pairs)
        together = jnp.concatenate([together, received], 0)
        distance //= 2
    return together


VMEM = pl.BlockSpec(memory_space=pltpu.VMEM)
SMEM = pl.BlockSpec(memory_space=pltpu.SMEM)
HBM = pl.BlockSpec(memory_space=pltpu.HBM)


def in_hbm(value):
    return pltpu.with_memory_space_constraint(value, pltpu.HBM)


def call(kernel, inputs, outputs, scratch, limit=8, places=None):
    return pl.pallas_call(
        kernel,
        in_specs=inputs,
        out_specs=places or jax.tree.map(lambda _: VMEM, outputs),
        out_shape=outputs,
        scratch_shapes=scratch,
        compiler_params=pltpu.CompilerParams(vmem_limit_bytes=limit << 20),
    )


def body(facets, sky_strips, prolate, subgrid_offset, owner, observed, vis_uv, vis_count):
    _, rows, width = sky_strips.shape
    slots, _, _, total = observed.shape
    subgrids = owner.shape[0]
    modulus = width * facets
    shape = jax.ShapeDtypeStruct
    weight = prolate.reshape(1, width)
    staged, mod, turns, live = call(
        functools.partial(setup_kernel, modulus, slots),
        [HBM] * 5,
        (
            shape(sky_strips.shape, jnp.bfloat16),
            shape((2, slots, facets, width), jnp.float32),
            shape((2, facets, 2 * POINTS), jnp.float32),
            shape((slots, rows, 128), jnp.int32),
        ),
        [
            pltpu.SMEM((subgrids,), jnp.int32),
            pltpu.SMEM((subgrids,), jnp.int32),
            pltpu.SMEM((slots,), jnp.int32),
            pltpu.VMEM((1, width), jnp.float32),
            pltpu.SemaphoreType.DMA((5,)),
        ],
    )(*(in_hbm(value) for value in (sky_strips, owner, subgrid_offset, vis_count, weight)))
    table = call(
        functools.partial(table_kernel, modulus),
        [],
        shape((2 * width, 2 * POINTS), jnp.bfloat16),
        [pltpu.VMEM((STEP, 2 * POINTS), jnp.float32)] * 2
        + [pltpu.VMEM((width // STEP, 2 * POINTS), jnp.float32)] * 2,
    )()
    back_table = call(
        functools.partial(back_table_kernel, modulus),
        [],
        shape((2 * POINTS, 2 * width), jnp.bfloat16),
        [pltpu.VMEM((BLOCK, width), jnp.float32)] * 2 + [pltpu.VMEM((FINE, width), jnp.float32)] * 2,
    )()
    pieces = [
        call(
            functools.partial(coarse_kernel, slot),
            [VMEM],
            (shape((BLOCK, total), jnp.bfloat16), shape((2, rows, total), jnp.float32)),
            [],
        )(vis_uv)
        for slot in range(slots)
    ]
    coarse = [piece[0] for piece in pieces]
    fine = [piece[1] for piece in pieces]
    sky = gather(sky_strips, staged, facets)
    points = call(
        functools.partial(grid_kernel, facets),
        [VMEM] * 4,
        shape((slots, 2 * FINE * rows, BLOCK), jnp.bfloat16),
        [
            pltpu.VMEM((slots * facets * rows, 2 * width), jnp.bfloat16),
            pltpu.VMEM((slots * facets * rows, 2 * POINTS), jnp.float32),
        ],
        16,
    )(sky, mod, turns, table)
    residual, update = call(
        functools.partial(visibility_kernel, slots),
        [VMEM] * (3 + 2 * slots),
        (
            shape((slots, 2, rows, total), jnp.bfloat16),
            shape((slots, rows, 2 * POINTS), jnp.bfloat16),
        ),
        [],
        16,
    )(points, live, observed, *coarse, *fine)

    back, lift, residual = call(
        functools.partial(plan_kernel, modulus),
        [HBM] * 3 + [VMEM],
        (
            shape((2, subgrids, width), jnp.float32),
            shape((2, rows, 2 * POINTS), jnp.float32),
            shape(residual.shape, residual.dtype),
        ),
        [
            pltpu.SMEM((subgrids,), jnp.int32),
            pltpu.SMEM((subgrids,), jnp.int32),
            pltpu.VMEM((1, width), jnp.float32),
            pltpu.SemaphoreType.DMA((4,)),
        ],
        places=(VMEM, VMEM, HBM),
    )(in_hbm(owner), in_hbm(subgrid_offset), in_hbm(weight), residual)
    updates = gather(update, update, facets).reshape(facets * slots, rows, 2 * POINTS)
    image = call(
        functools.partial(image_kernel, facets, slots),
        [SMEM] + [VMEM] * 4,
        shape((2, rows, width), jnp.float32),
        [
            pltpu.VMEM((subgrids * rows, 2 * POINTS), jnp.bfloat16),
            pltpu.SMEM((facets,), jnp.int32),
            pltpu.SMEM((subgrids,), jnp.int32),
        ],
        16,
    )(owner, updates, back, lift, back_table)
    return residual, image


def local(facets, *arguments):
    return body(facets, *arguments)


def solution(mesh):
    in_specs = (
        P(None, "groups", "facet"),
        P(),
        P(),
        P(),
        P(("groups", "facet"), None, None, None),
        P(("groups", "facet"), None),
        P(("groups", "facet")),
    )
    out_specs = (P(("groups", "facet"), None, None, None), P(None, "groups", "facet"))
    return jax.shard_map(
        functools.partial(local, mesh.shape["facet"]),
        mesh=mesh,
        in_specs=in_specs,
        out_specs=out_specs,
        check_vma=False,
    )
```

```python
import functools
import math

import jax
import jax.numpy as jnp
from jax import lax
from jax.experimental import pallas as pl
from jax.experimental.pallas import tpu as pltpu
from jax.sharding import PartitionSpec as P


POINTS = 512
FINE = 8
COARSE = POINTS // FINE
BLOCK = 2 * COARSE
ROOT = 8
SPLIT = 2
STEP = 64
FAR = 4
CHUNK = 512

COS = (
    0.9999999890590217, -4.934801124863452, 4.058694841243232, -1.3351584301691248,
    0.23502980840046309, -0.025358983639642813, 0.001593910683444594,
)
SIN = (
    3.14159265125575, -5.167712550664621, 2.550160355805489, -0.5992423074495862,
    0.08208188864038139, -0.00727531575291481, 0.00039528045693413335,
)


def horner(coefficients, z):
    total = coefficients[-1] * z + coefficients[-2]
    for value in coefficients[-3::-1]:
        total = total * z + value
    return total


def turn(t):
    y = 2.0 * (t - jnp.floor(t + 0.5))
    z = y * y
    return horner(COS, z), horner(SIN, z) * y


def modular(first, second, modulus):
    if modulus & (modulus - 1) == 0:
        return (first * second) & (modulus - 1)
    upper = second // 256
    lower = second % 256
    return (first * lower % modulus + first * upper % modulus * 256 % modulus) % modulus


def iota(shape, axis):
    return lax.broadcasted_iota(jnp.int32, shape, axis)


def column_points(shape):
    column = iota(shape, 1)
    return (column % COARSE) * FINE + column // BLOCK, (column // COARSE) % 2


def position_of(facet, me, facets):
    far = min(FAR, facets)
    near = facets // far
    bits = near.bit_length() - 1
    flipped = facet * 0
    for bit in range(bits):
        flipped = flipped | ((((facet ^ me) >> bit) & 1) << (bits - 1 - bit))
    return (me // near - facet // near + far) % far + far * flipped


def swap(block):
    return pltpu.roll(block, COARSE, 1)


def blocks_of(value):
    return [value[:, b * BLOCK : (b + 1) * BLOCK] for b in range(FINE)]


def find_offsets(me, owner_ref, offset_ref, slots):
    def find(index, carry):
        held, offsets = carry
        mine = owner_ref[index] == me
        offsets = tuple(
            jnp.where(mine & (held == slot), offset_ref[index], offsets[slot]) for slot in range(slots)
        )
        return held + mine.astype(jnp.int32), offsets

    zero = jnp.int32(0)
    return lax.fori_loop(0, owner_ref.shape[0], find, (zero, (zero,) * slots))


def fraction_of(first, second, modulus):
    return modular(first, second, modulus).astype(jnp.float32) * (1.0 / modulus)


def fetch(copies, semaphores):
    started = [
        pltpu.make_async_copy(source, target, semaphores.at[index])
        for index, (source, target) in enumerate(copies)
    ]
    for copy in started:
        copy.start()
    return started


def wait_for(copies):
    for copy in copies:
        copy.wait()


def setup_kernel(
    modulus,
    slots,
    owner_hbm,
    offset_hbm,
    count_hbm,
    prolate_hbm,
    sky_hbm,
    uv_hbm,
    observed_hbm,
    mod_ref,
    turn_ref,
    live_ref,
    sky_ref,
    uv_ref,
    observed_ref,
    owner_ref,
    offset_ref,
    count_ref,
    prolate_ref,
    semaphores,
):
    copies = fetch(
        (
            (owner_hbm, owner_ref),
            (offset_hbm, offset_ref),
            (count_hbm, count_ref),
            (prolate_hbm, prolate_ref),
            (sky_hbm, sky_ref),
            (uv_hbm, uv_ref),
            (observed_hbm, observed_ref),
        ),
        semaphores,
    )
    wait_for(copies[:4])
    me = lax.axis_index("facet")
    facets, width = mod_ref.shape[2:]
    held, offsets = find_offsets(me, owner_ref, offset_ref, slots)
    weight = prolate_ref[...]

    across = iota((facets, width), 0) * width + iota((facets, width), 1)
    for slot in range(slots):
        c, s = turn(fraction_of(across, offsets[slot], modulus))
        mod_ref[0, slot] = c * weight
        mod_ref[1, slot] = s * weight
        live_ref[slot] = jnp.full(live_ref.shape[1:], jnp.where(slot < held, count_ref[slot], 0))

    points, part = column_points(turn_ref.shape[1:])
    c, s = turn(fraction_of(iota(points.shape, 0), points, facets * SPLIT))
    scale = 1.0 / math.sqrt(modulus)
    turn_ref[0] = c * scale
    turn_ref[1] = jnp.where(part == 0, -s, s) * scale
    wait_for(copies[4:])


def plan_kernel(
    modulus,
    owner_hbm,
    offset_hbm,
    prolate_hbm,
    residual_ref,
    back_ref,
    lift_ref,
    residual_hbm,
    owner_ref,
    offset_ref,
    prolate_ref,
    semaphores,
):
    leaving = pltpu.make_async_copy(residual_ref, residual_hbm, semaphores.at[3])
    leaving.start()
    wait_for(
        fetch(
            ((owner_hbm, owner_ref), (offset_hbm, offset_ref), (prolate_hbm, prolate_ref)), semaphores
        )
    )
    me = lax.axis_index("facet")
    facets = lax.axis_size("facet")
    subgrids, width = back_ref.shape[1:]
    row = iota((subgrids, 128), 0)

    def place_offset(index, placed):
        return jnp.where(row == index, offset_ref[index], placed)

    column = lax.fori_loop(0, subgrids, place_offset, jnp.zeros(row.shape, jnp.int32), unroll=True)
    across = me * width + iota((subgrids, width), 1)
    c, s = turn(fraction_of(across, jnp.concatenate([column] * (width // 128), 1), modulus))
    weight = prolate_ref[...] * (1.0 / math.sqrt(subgrids * POINTS))
    back_ref[0] = c * weight
    back_ref[1] = s * weight

    points, part = column_points(lift_ref.shape[1:])
    c, s = turn(fraction_of(me * SPLIT + iota(points.shape, 0), points, facets * SPLIT))
    lift_ref[0] = c
    lift_ref[1] = jnp.where(part == 0, -s, s)
    leaving.wait()


def table_kernel(modulus, table_ref, v_re, v_im, u_re, u_im):
    width = table_ref.shape[0] // 2
    points, part = column_points(v_re.shape)
    fraction = fraction_of(iota(v_re.shape, 0), points, modulus)
    v_re[...], v_im[...] = turn(fraction + 0.25 * part.astype(jnp.float32))
    points, _ = column_points(u_re.shape)
    u_re[...], u_im[...] = turn(fraction_of(iota(u_re.shape, 0) * STEP, points, modulus))

    def table_step(step, _):
        c = u_re[pl.ds(step, 1), :]
        s = u_im[pl.ds(step, 1), :]
        row = pl.multiple_of(step * STEP, STEP)
        table_ref[pl.ds(row, STEP), :] = (v_re[...] * c - v_im[...] * s).astype(jnp.bfloat16)
        table_ref[pl.ds(width + row, STEP), :] = (v_re[...] * s + v_im[...] * c).astype(jnp.bfloat16)
        return 0

    lax.fori_loop(0, width // STEP, table_step, 0)


def back_table_kernel(modulus, table_ref, v_re, v_im, u_re, u_im):
    width = table_ref.shape[1] // 2
    row = iota(v_re.shape, 0)
    fraction = fraction_of(iota(v_re.shape, 1), row % COARSE * FINE, modulus)
    v_re[...], v_im[...] = turn(fraction + 0.25 * (row // COARSE).astype(jnp.float32))
    u_re[...], u_im[...] = turn(fraction_of(iota(u_re.shape, 1), iota(u_re.shape, 0), modulus))

    def table_step(b, _):
        c = u_re[pl.ds(b, 1), :]
        s = u_im[pl.ds(b, 1), :]
        at = pl.ds(pl.multiple_of(b * BLOCK, BLOCK), BLOCK)
        table_ref[at, :width] = (v_re[...] * c - v_im[...] * s).astype(jnp.bfloat16)
        table_ref[at, width:] = (v_re[...] * s + v_im[...] * c).astype(jnp.bfloat16)
        return 0

    lax.fori_loop(0, FINE, table_step, 0)


def combine(products, rows, halves):
    count = products.shape[0] // (2 * rows)
    return [
        swap(products[(count + b) * rows : (count + b + 1) * rows]) + products[b * rows : (b + 1) * rows] * halves
        for b in range(count)
    ]


def split(value):
    part = value.shape[1] // SPLIT
    return jnp.concatenate([value[:, index * part : (index + 1) * part] for index in range(SPLIT)], 0)


def half_signs(rows):
    return jnp.where(iota((rows, BLOCK), 1) < COARSE, jnp.float32(1.0), jnp.float32(-1.0))


def powers(c, s, bits):
    re = jnp.where(bits[0], c, 1.0)
    im = jnp.where(bits[0], s, 0.0)
    for bit in bits[1:]:
        c, s = c * c - s * s, 2.0 * c * s
        re, im = (
            jnp.where(bit, re * c - im * s, re),
            jnp.where(bit, re * s + im * c, im),
        )
    return re, im


def observe_kernel(
    slot, uv_ref, live_ref, observed_ref, coarse_ref, fine_ref, seen_ref, lags_ref, step_c, step_s, back_c, back_s, root_c, root_s, packed
):
    count, wide = packed.shape
    rows = observed_ref.shape[2]
    for row in range(count):
        packed[row : row + 1, :] = uv_ref[slot : slot + 1, row * wide : (row + 1) * wide]
    u = packed[...]
    fine_ref[0], fine_ref[1] = turn(u * (1.0 / POINTS))
    step_c[...], step_s[...] = turn(u * (FINE * ROOT / POINTS))
    back_c[...], back_s[...] = turn(u)
    root_c[...], root_s[...] = turn(u * (FINE / POINTS))
    chunk = min(CHUNK, wide)
    bits = [(iota((ROOT, chunk), 0) >> bit) % 2 == 1 for bit in range(3)]
    live = jnp.concatenate([live_ref[slot]] * (chunk // live_ref.shape[2]), 1)
    gathered = jnp.zeros((2 * FINE * (rows + 2), BLOCK), jnp.float32)

    for row in range(count):
        for start in range(0, wide, chunk):
            here = slice(start, start + chunk)
            at = slice(row * wide + start, row * wide + start + chunk)

            def spread(ref):
                return jnp.broadcast_to(ref[row : row + 1, here], (ROOT, chunk))

            re, im = powers(spread(root_c), spread(root_s), bits)
            c, s = spread(step_c), spread(step_s)
            cosines, sines = [], []
            for step in range(ROOT):
                cosines.append(re)
                sines.append(im)
                if step + 1 < ROOT:
                    re, im = re * c - im * s, re * s + im * c
            coarse = jnp.concatenate(cosines + sines, 0).astype(jnp.bfloat16)
            coarse_ref[:, at] = coarse

            alive = row * wide + start + iota((rows, chunk), 1) < live
            c = jnp.broadcast_to(fine_ref[0, row : row + 1, here], (rows, chunk))
            s = jnp.broadcast_to(fine_ref[1, row : row + 1, here], (rows, chunk))
            re = jnp.where(alive, observed_ref[slot, 0, :, at], 0.0)
            im = jnp.where(alive, observed_ref[slot, 1, :, at], 0.0)
            all_re, all_im = [re], [im]
            for _ in range(1, FINE):
                re, im = re * c + im * s, im * c - re * s
                all_re.append(re)
                all_im.append(im)
            re, im = powers(c, -s, bits)
            re = jnp.where(alive, re, 0.0)
            im = jnp.where(alive, im, 0.0)
            c, s = spread(back_c), spread(back_s)
            all_re += [re * c - im * s, re]
            all_im += [re * s + im * c, im]
            gathered = gathered + lax.dot_general(
                jnp.concatenate(all_re + all_im, 0).astype(jnp.bfloat16),
                coarse,
                (((1,), (1,)), ((), ())),
                preferred_element_type=jnp.float32,
            )

    blocks = combine(gathered, rows, half_signs(rows))
    for b in range(FINE):
        seen_ref[:, b * BLOCK : (b + 1) * BLOCK] = blocks[b]
    before, after = blocks[FINE:]
    first = iota((FINE, BLOCK), 1) < COARSE
    lags_ref[0] = jnp.where(first, before, swap(after))
    lags_ref[1] = jnp.where(first, swap(before), after)


def toeplitz_kernel(slots, *refs):
    first = iota((COARSE, BLOCK), 1) < COARSE

    def slant(ref, part, row, shift):
        line = jnp.broadcast_to(ref[part, row : row + 1, :], (COARSE, BLOCK))
        return pltpu.roll(line, shift, 1, stride=1, stride_axis=0)

    for slot in range(slots):
        lags_ref, matrix_ref = refs[slot], refs[slots + slot]
        for place in range(2 * FINE - 1):
            beta = place - (FINE - 1)
            row, late = (beta, 0) if beta >= 0 else (beta + FINE, 1)
            upper = jnp.where(
                first, slant(lags_ref, 0, row, COARSE + late), slant(lags_ref, 1, row, late)
            )
            lower = jnp.where(
                first, -slant(lags_ref, 1, row, COARSE + late), slant(lags_ref, 0, row, late)
            )
            value = jnp.concatenate([upper, lower], 0)
            high = value.astype(jnp.bfloat16)
            at = slice(place * BLOCK, (place + 1) * BLOCK)
            matrix_ref[:BLOCK, at] = high
            matrix_ref[BLOCK:, at] = (value - high.astype(jnp.float32)).astype(jnp.bfloat16)
        matrix_ref[:, (2 * FINE - 1) * BLOCK :] = jnp.zeros((2 * BLOCK, BLOCK), jnp.bfloat16)


def grid_kernel(facets, total, sky_ref, mod_ref, turn_ref, table_ref, *refs):
    me = lax.axis_index("facet")
    slots = mod_ref.shape[1]
    seen_refs, matrix_refs = refs[:slots], refs[slots : 2 * slots]
    points_ref, update_ref, lhs, raw = refs[2 * slots :]
    part = sky_ref.shape[3] // SPLIT
    rows = sky_ref.shape[2]

    for slot in range(slots):

        def modulate(facet, _):
            c = mod_ref[0, slot, pl.ds(facet, 1), :]
            s = mod_ref[1, slot, pl.ds(facet, 1), :]
            position = position_of(facet, me, facets)
            re = sky_ref[position, 0].astype(jnp.float32)
            im = sky_ref[position, 1].astype(jnp.float32)
            row = pl.multiple_of((slot * facets + facet) * SPLIT * rows, SPLIT * rows)
            at = pl.ds(row, SPLIT * rows)
            lhs[at, :part] = split(re * c + im * s).astype(jnp.bfloat16)
            lhs[at, part:] = split(im * c - re * s).astype(jnp.bfloat16)
            return 0

        lax.fori_loop(0, facets, modulate, 0, unroll=True)

    raw[...] = jnp.dot(lhs[...], table_ref[...], preferred_element_type=jnp.float32)
    halves = half_signs(rows)

    for slot in range(slots):

        def add_facet(position, carry):
            straight, crossed = carry
            row = pl.multiple_of((slot * facets * SPLIT + position) * rows, rows)
            value = raw[pl.ds(row, rows), :]
            return (
                straight + value * turn_ref[0, pl.ds(position, 1), :],
                crossed + value * turn_ref[1, pl.ds(position, 1), :],
            )

        empty = jnp.zeros((rows, FINE * BLOCK), jnp.float32)
        straight, crossed = lax.fori_loop(0, facets * SPLIT, add_facet, (empty, empty), unroll=True)
        grid = [
            (first + swap(second)).astype(jnp.bfloat16).astype(jnp.float32)
            for first, second in zip(blocks_of(straight), blocks_of(crossed))
        ]
        points_ref[slot] = jnp.concatenate(
            [block * halves for block in grid] + [swap(block) for block in grid], 0
        ).astype(jnp.bfloat16)

        stacked = jnp.concatenate(grid, 0).astype(jnp.bfloat16)
        products = jnp.dot(
            jnp.concatenate([stacked, stacked], 1), matrix_refs[slot][...], preferred_element_type=jnp.float32
        )
        for after in range(FINE):
            model = sum(
                products[
                    b * rows : (b + 1) * rows,
                    (after - b + FINE - 1) * BLOCK : (after - b + FINE) * BLOCK,
                ]
                for b in range(FINE)
            )
            at = slice(after * BLOCK, (after + 1) * BLOCK)
            update_ref[slot, :, at] = (
                (seen_refs[slot][:, at] - model * (1.0 / math.sqrt(POINTS))) * (1.0 / math.sqrt(total))
            ).astype(jnp.bfloat16)


def residual_kernel(slots, points_ref, live_ref, observed_ref, *refs):
    coarse_refs, fine_refs = refs[:slots], refs[slots : 2 * slots]
    residual_ref = refs[2 * slots]
    _, _, rows, total = observed_ref.shape
    chunk = min(CHUNK, total)

    for slot in range(slots):
        points_lhs = points_ref[slot]
        live = jnp.concatenate([live_ref[slot]] * (chunk // live_ref.shape[2]), 1)
        wide = fine_refs[slot].shape[2]
        for start in range(0, total, chunk):
            at = slice(start, start + chunk)
            row, here = start // wide, slice(start % wide, start % wide + chunk)
            c = jnp.broadcast_to(fine_refs[slot][0, row : row + 1, here], (rows, chunk))
            s = jnp.broadcast_to(fine_refs[slot][1, row : row + 1, here], (rows, chunk))
            terms = jnp.dot(points_lhs, coarse_refs[slot][:, at], preferred_element_type=jnp.float32)
            half = FINE * rows
            re = terms[half - rows : half]
            im = terms[2 * half - rows :]
            for b in range(FINE - 2, -1, -1):
                re, im = (
                    terms[b * rows : (b + 1) * rows] + (re * c - im * s),
                    terms[half + b * rows : half + (b + 1) * rows] + (re * s + im * c),
                )
            scale = 1.0 / math.sqrt(POINTS)
            alive = start + iota((rows, chunk), 1) < live
            re = jnp.where(alive, observed_ref[slot, 0, :, at] - re * scale, 0.0)
            im = jnp.where(alive, observed_ref[slot, 1, :, at] - im * scale, 0.0)
            residual_ref[slot, 0, :, at] = re.astype(jnp.bfloat16)
            residual_ref[slot, 1, :, at] = im.astype(jnp.bfloat16)


def image_kernel(
    facets,
    slots,
    owner_ref,
    update_ref,
    back_ref,
    lift_ref,
    table_ref,
    image_ref,
    lhs,
    taken,
    place,
):
    me = lax.axis_index("facet")
    subgrids = owner_ref.shape[0]
    rows = update_ref.shape[1]
    width = image_ref.shape[2]

    def clear(index, _):
        taken[index] = 0
        return 0

    lax.fori_loop(0, facets, clear, 0, unroll=True)

    def assign(index, _):
        holder = owner_ref[index]
        rank = taken[holder]
        taken[holder] = rank + 1
        place[index] = position_of(holder, me, facets) * slots + rank
        return 0

    lax.fori_loop(0, subgrids, assign, 0, unroll=True)

    def lift(index, _):
        value = update_ref[place[index]].astype(jnp.float32)
        turned = jnp.concatenate([swap(block) for block in blocks_of(value)], 1)
        at = pl.ds(pl.multiple_of(index * SPLIT * rows, SPLIT * rows), SPLIT * rows)
        lhs[at, :] = jnp.concatenate(
            [
                value * lift_ref[0, part : part + 1, :] + turned * lift_ref[1, part : part + 1, :]
                for part in range(SPLIT)
            ],
            0,
        ).astype(jnp.bfloat16)
        return 0

    lax.fori_loop(0, subgrids, lift, 0, unroll=True)
    back = jnp.dot(lhs[...], table_ref[...], preferred_element_type=jnp.float32)
    wide = width // SPLIT
    for part in range(SPLIT):
        at = slice(part * wide, (part + 1) * wide)
        out_re = jnp.zeros((rows, wide), jnp.float32)
        out_im = jnp.zeros((rows, wide), jnp.float32)
        for index in range(subgrids):
            first = (index * SPLIT + part) * rows
            re = back[first : first + rows, :wide]
            im = back[first : first + rows, wide:]
            c = back_ref[0, index : index + 1, at]
            s = back_ref[1, index : index + 1, at]
            out_re = out_re + (re * c - im * s)
            out_im = out_im + (re * s + im * c)
        image_ref[0, :, at] = out_re
        image_ref[1, :, at] = out_im


def gather(value, staged, facets):
    far = min(FAR, facets)
    near = facets // far
    pieces = [staged[None]]
    for step in range(1, far):
        pairs = [(index, (index + step * near) % facets) for index in range(facets)]
        pieces.append(lax.ppermute(value, "facet", pairs)[None])
    together = jnp.concatenate(pieces, 0)
    distance = near // 2
    while distance:
        pairs = [(index, index ^ distance) for index in range(facets)]
        received = lax.ppermute(together, "facet", pairs)
        together = jnp.concatenate([together, received], 0)
        distance //= 2
    return together


VMEM = pl.BlockSpec(memory_space=pltpu.VMEM)
SMEM = pl.BlockSpec(memory_space=pltpu.SMEM)
HBM = pl.BlockSpec(memory_space=pltpu.HBM)


def in_hbm(value):
    return pltpu.with_memory_space_constraint(value, pltpu.HBM)


def call(kernel, inputs, outputs, scratch, limit=8, places=None):
    return pl.pallas_call(
        kernel,
        in_specs=inputs,
        out_specs=places or jax.tree.map(lambda _: VMEM, outputs),
        out_shape=outputs,
        scratch_shapes=scratch,
        compiler_params=pltpu.CompilerParams(vmem_limit_bytes=limit << 20),
    )


def body(facets, sky_strips, prolate, subgrid_offset, owner, observed, vis_uv, vis_count):
    _, rows, width = sky_strips.shape
    slots, _, _, total = observed.shape
    subgrids = owner.shape[0]
    modulus = width * facets
    shape = jax.ShapeDtypeStruct
    weight = prolate.reshape(1, width)
    mod, turns, live, staged, uv, visibilities = call(
        functools.partial(setup_kernel, modulus, slots),
        [HBM] * 7,
        (
            shape((2, slots, facets, width), jnp.float32),
            shape((2, facets * SPLIT, 2 * POINTS), jnp.float32),
            shape((slots, rows, 128), jnp.int32),
            shape(sky_strips.shape, sky_strips.dtype),
            shape(vis_uv.shape, vis_uv.dtype),
            shape(observed.shape, observed.dtype),
        ),
        [
            pltpu.SMEM((subgrids,), jnp.int32),
            pltpu.SMEM((subgrids,), jnp.int32),
            pltpu.SMEM((slots,), jnp.int32),
            pltpu.VMEM((1, width), jnp.float32),
            pltpu.SemaphoreType.DMA((7,)),
        ],
    )(*(in_hbm(value) for value in (owner, subgrid_offset, vis_count, weight, sky_strips, vis_uv, observed)))
    table = call(
        functools.partial(table_kernel, modulus),
        [],
        shape((2 * width // SPLIT, 2 * POINTS), jnp.bfloat16),
        [pltpu.VMEM((STEP, 2 * POINTS), jnp.float32)] * 2
        + [pltpu.VMEM((width // SPLIT // STEP, 2 * POINTS), jnp.float32)] * 2,
    )()
    back_table = call(
        functools.partial(back_table_kernel, modulus),
        [],
        shape((2 * POINTS, 2 * width // SPLIT), jnp.bfloat16),
        [pltpu.VMEM((BLOCK, width // SPLIT), jnp.float32)] * 2
        + [pltpu.VMEM((FINE, width // SPLIT), jnp.float32)] * 2,
    )()
    pieces = [
        call(
            functools.partial(observe_kernel, slot),
            [VMEM] * 3,
            (
                shape((BLOCK, total), jnp.bfloat16),
                shape((2, 8, total // 8), jnp.float32),
                shape((rows, 2 * POINTS), jnp.float32),
                shape((2, FINE, BLOCK), jnp.float32),
            ),
            [pltpu.VMEM((8, total // 8), jnp.float32)] * 7,
        )(uv, live, visibilities)
        for slot in range(slots)
    ]
    coarse, fine, seen, lags = zip(*pieces)
    matrices = call(
        functools.partial(toeplitz_kernel, slots),
        [VMEM] * slots,
        (shape((2 * BLOCK, 2 * FINE * BLOCK), jnp.bfloat16),) * slots,
        [],
    )(*lags)
    sky = gather(sky_strips, staged, facets)
    points, update = call(
        functools.partial(grid_kernel, facets, total),
        [VMEM] * (4 + 2 * slots),
        (
            shape((slots, 2 * FINE * rows, BLOCK), jnp.bfloat16),
            shape((slots, rows, 2 * POINTS), jnp.bfloat16),
        ),
        [
            pltpu.VMEM((slots * facets * SPLIT * rows, 2 * width // SPLIT), jnp.bfloat16),
            pltpu.VMEM((slots * facets * SPLIT * rows, 2 * POINTS), jnp.float32),
        ],
        16,
    )(sky, mod, turns, table, *seen, *matrices)
    residual = call(
        functools.partial(residual_kernel, slots),
        [VMEM] * (3 + 2 * slots),
        shape((slots, 2, rows, total), jnp.bfloat16),
        [],
        16,
    )(points, live, visibilities, *coarse, *fine)

    back, lift, residual = call(
        functools.partial(plan_kernel, modulus),
        [HBM] * 3 + [VMEM],
        (
            shape((2, subgrids, width), jnp.float32),
            shape((2, SPLIT, 2 * POINTS), jnp.float32),
            shape(residual.shape, residual.dtype),
        ),
        [
            pltpu.SMEM((subgrids,), jnp.int32),
            pltpu.SMEM((subgrids,), jnp.int32),
            pltpu.VMEM((1, width), jnp.float32),
            pltpu.SemaphoreType.DMA((4,)),
        ],
        places=(VMEM, VMEM, HBM),
    )(in_hbm(owner), in_hbm(subgrid_offset), in_hbm(weight), residual)
    updates = gather(update, update, facets).reshape(-1, rows, 2 * POINTS)
    image = call(
        functools.partial(image_kernel, facets, slots),
        [SMEM] + [VMEM] * 4,
        shape((2, rows, width), jnp.float32),
        [
            pltpu.VMEM((subgrids * SPLIT * rows, 2 * POINTS), jnp.bfloat16),
            pltpu.SMEM((facets,), jnp.int32),
            pltpu.SMEM((subgrids,), jnp.int32),
        ],
        16,
    )(owner, updates, back, lift, back_table)
    return residual, image


def local(facets, *arguments):
    return body(facets, *arguments)


def solution(mesh):
    in_specs = (
        P(None, "groups", "facet"),
        P(),
        P(),
        P(),
        P(("groups", "facet"), None, None, None),
        P(("groups", "facet"), None),
        P(("groups", "facet")),
    )
    out_specs = (P(("groups", "facet"), None, None, None), P(None, "groups", "facet"))
    return jax.shard_map(
        functools.partial(local, mesh.shape["facet"]),
        mesh=mesh,
        in_specs=in_specs,
        out_specs=out_specs,
        check_vma=False,
    )
```
